32 devices in a mesh: tm: 8 (over z, x), chan: 4 (over y, core).
Axes of the slice: x: 2, y: 2, z: 4, core: 2. Of those that a mesh axis runs over, the one named last changes fastest.
Arguments:
- surveillance: bfloat16 [128, 1024, 256], P(('chan', 'tm')), parts along dimension 0, may hold values from -6 to 6
- ref_samples: bfloat16 [32, 1040, 256], P('tm'), may hold values from -6 to 6
- block_ids: int32 [32], P('tm'), may hold values from 0 to 31, each once
- walk: int32 [32], P('tm'), may hold values from 0 to 63
- cfar_guard: int32 [2048], P('tm'), may hold values from 1 to 8
- cfar_window: int32 [2048], P('tm'), may hold values from 1 to 16
Outputs:
- detection: float32 [8192, 512], P(('chan', 'tm')), parts along dimension 0
The draws below stay inside these ranges and needn't reach their ends.
There are 4 independent parts, one for each index of `chan`. The reference program is written for one: setup_inputs(seed, part) draws one part's arguments, and reference() takes and returns one part's arrays. A program takes and returns all parts, laid end to end along the dimension named above; an argument that names none is the same for every part. Nothing has to cross between parts.
Inputs may be any that keep to these rules, and one draw needn't show every extreme that they name: block_ids names each of 0 to 31 exactly once.
All inputs are finite; a program needn't handle non-finite values.
Results may differ from the reference program's by a relative error of at most 0.0003.
Values sent between devices are 32-bit elements; how exact they have to be, the bound alone decides.
A program may use at most 64 MiB of HBM per device.

```python
import math
import jax
import jax.numpy as jnp
from jax import lax

D = 2048
DOP = 512
SEGS = 64
GUARD_MAX = 8
WIN_MAX = 16
WALK = 64
NB = 32
L = 131072


def plant(values, own_key, smallest, high):
    place = [jax.random.randint(jax.random.fold_in(own_key, axis), (), 0, length) for axis, length in enumerate(values.shape)]
    main_axis = values.shape.index(max(values.shape))
    neighbour = place[:main_axis] + [(place[main_axis] + 1) % values.shape[main_axis]] + place[main_axis + 1:]
    return values.at[tuple(place)].set(smallest).at[tuple(neighbour)].set(high)


def levels(key, shape, cuts, low, largest):
    gain = 1.0
    for dim, shards_of in cuts:
        heights = jax.random.uniform(jax.random.fold_in(jax.random.fold_in(key, 6), dim), (shards_of,), jnp.float32, low / len(cuts), largest / len(cuts))
        gain = gain * jnp.repeat(jnp.exp(heights), shape[dim] // shards_of).reshape((-1,) + (1,) * (len(shape) - 1 - dim))
    return gain


def gaussian(key, shape, scale, bound, pieces=(), kind=jnp.bfloat16):
    result = jax.random.normal(key, shape, jnp.float32) * scale
    if len(pieces) > 0:
        result = levels(key, shape, pieces, -0.22, 0.18) * result
    return jnp.clip(result, min=-bound, max=bound).astype(kind)


def setup_inputs(seed: int = 0, part: int = 0) -> dict:
    keys = jax.random.split(jax.random.key(seed), 7)
    part_splits = jax.random.split(jax.random.fold_in(keys[6], part), 7)
    surveillance = gaussian(part_splits[0], (NB, L // 128, 256), 1.0, 6.0, ((0, 8),))
    ref_samples = gaussian(keys[1], (NB, (L + D) // 128, 256), 1.0, 6.0, ((0, 8),))
    block_ids = jax.random.permutation(keys[2], NB).astype(jnp.int32)
    walk = plant(jax.random.randint(keys[3], (NB,), 0, WALK), jax.random.fold_in(keys[3], 1), 0, WALK - 1).astype(jnp.int32)
    cfar_guard = plant(jax.random.randint(keys[4], (D,), 1, GUARD_MAX + 1), jax.random.fold_in(keys[4], 1), 1, GUARD_MAX).astype(jnp.int32)
    cfar_window = plant(jax.random.randint(keys[5], (D,), 1, WIN_MAX + 1), jax.random.fold_in(keys[5], 1), 1, WIN_MAX).astype(jnp.int32)
    return dict(surveillance=surveillance, ref_samples=ref_samples, block_ids=block_ids, walk=walk, cfar_guard=cfar_guard, cfar_window=cfar_window)


HIGH = lax.Precision.HIGHEST

def unpack(packed):
    count = packed.shape[0]
    real_part = packed[:, :, :128].astype(jnp.float32).reshape(count, -1)
    imag_part = packed[:, :, 128:].astype(jnp.float32).reshape(count, -1)
    return lax.complex(real_part, imag_part)

def correlate(item):
    surv_line, ref_line, shift = item
    segment = surv_line.reshape(SEGS, D)
    padded = jnp.concatenate([segment, jnp.zeros_like(segment)], axis=1)
    first = ref_line[:SEGS * D].reshape(SEGS, D)
    second = ref_line[D:].reshape(SEGS, D)
    window = jnp.concatenate([first, second], axis=1)
    spectrum = lax.optimization_barrier(jnp.sum(jnp.fft.fft(padded, axis=1) * jnp.conj(jnp.fft.fft(window, axis=1)), axis=0))
    lagged = jnp.fft.ifft(spectrum)
    picked = lax.dynamic_slice_in_dim(lagged, (D - shift).astype(jnp.int32), D)
    keep = jnp.arange(D, dtype=jnp.int32) >= shift
    return (jnp.where(keep, jnp.real(picked), 0.0), jnp.where(keep, jnp.imag(picked), 0.0))

def reference(surveillance, ref_samples, block_ids, walk, cfar_guard, cfar_window):
    real_c, imag_c = lax.map(correlate, (unpack(surveillance), unpack(ref_samples), walk))
    norm = 1.0 / math.sqrt(NB * SEGS * D)
    freq = jnp.arange(DOP, dtype=jnp.int32)
    theta = 2.0 * math.pi / DOP * (block_ids[:, None] * freq[None, :] % DOP).astype(jnp.float32)
    cos_table = jnp.cos(theta)
    sin_table = jnp.sin(theta)
    amp_re = (jnp.dot(real_c.T, cos_table, precision=HIGH) + jnp.dot(imag_c.T, sin_table, precision=HIGH)) * norm
    amp_im = (jnp.dot(imag_c.T, cos_table, precision=HIGH) - jnp.dot(real_c.T, sin_table, precision=HIGH)) * norm
    power = amp_re * amp_re + amp_im * amp_im
    floor = lax.optimization_barrier(jnp.sum(real_c * real_c + imag_c * imag_c, axis=0)) / (NB * SEGS * D)
    guard = cfar_guard
    width = cfar_window
    reach = GUARD_MAX + WIN_MAX
    padded = jnp.pad(power, ((reach, reach), (0, 0)))
    valid = jnp.pad(jnp.ones((D,), jnp.float32), (reach, reach))
    delay_sum = jnp.zeros_like(power)
    doppler_sum = jnp.zeros_like(power)
    count = jnp.zeros((D,), jnp.float32)
    for step in range(1, reach + 1):
        active = ((step > guard) & (step <= guard + width)).astype(jnp.float32)
        delay_sum = delay_sum + active[:, None] * (padded[reach + step:reach + step + D] + padded[reach - step:reach - step + D])
        count = count + active * (valid[reach + step:reach + step + D] + valid[reach - step:reach - step + D])
        doppler_sum = doppler_sum + active[:, None] * (jnp.roll(power, -step, axis=1) + jnp.roll(power, step, axis=1))
    noise = (delay_sum + doppler_sum) / (count[:, None] + 2.0 * width.astype(jnp.float32)[:, None])
    return (power - floor[:, None]) / (0.25 + noise)
```

```python
import functools
import math

import numpy as np
import jax
import jax.numpy as jnp
from jax import lax
from jax.experimental import pallas as pl
from jax.experimental.pallas import tpu as pltpu
from jax.sharding import PartitionSpec as P

D = 2048
DOP = 512
SEGS = 64
GUARD_MAX = 8
WIN_MAX = 16
REACH = GUARD_MAX + WIN_MAX
LANES = 128
SEG_ROWS = D // LANES
CHUNK = SEG_ROWS * SEG_ROWS
MAP_LIMIT = 24 * 1024 * 1024
VMEM_LIMIT = 53 * 1024 * 1024
MESH = pl.DeviceIdType.MESH
F32 = jnp.float32
BF16 = jnp.bfloat16


def window_rows(span):
    return max(s % LANES + span + 2 * REACH for s in range(0, D, span)) // LANES + 1


def iota(shape, dim):
    return lax.broadcasted_iota(jnp.int32, shape, dim)


def split(x):
    high = x.astype(BF16)
    return high, (x - high.astype(F32)).astype(BF16)


def mm(a, b, dims=((1,), (0,))):
    return lax.dot_general(a, b, (dims, ((), ())), preferred_element_type=F32)


def mm3(a, high, low):
    a_high, a_low = split(a)
    return mm(a_high, high) + (mm(a_low, high) + mm(a_high, low))


def correlate_kernel(
    span, walk_hbm, ids_hbm, s_hbm, e_hbm, out_ref,
    walk_ref, ids_ref, s_ref, e_ref, lhs_ref, rhs_ref, diag_ref, send, got,
    small_sem, in_sem, send_sem, recv_sem,
):
    blocks, rows_all = s_hbm.shape[:2]
    chunks = rows_all // CHUNK
    devices = got.shape[0]
    rows_sent = window_rows(span)
    me = lax.axis_index("tm")
    barrier = pltpu.get_barrier_semaphore()
    peers = [lax.rem(me + k, devices) for k in range(1, devices)]
    small = [
        pltpu.make_async_copy(walk_hbm, walk_ref, small_sem.at[0]),
        pltpu.make_async_copy(ids_hbm, ids_ref, small_sem.at[1]),
    ]
    loads = [
        [
            pltpu.make_async_copy(s_hbm.at[j], s_ref.at[j], in_sem.at[j, 0]),
            pltpu.make_async_copy(e_hbm.at[j], e_ref.at[j], in_sem.at[j, 1]),
        ]
        for j in range(blocks)
    ]
    for copy in loads[0] + small + sum(loads[1:], []):
        copy.start()
    for peer in peers:
        pl.semaphore_signal(barrier, inc=1, device_id={"tm": peer}, device_id_type=MESH)
    send[...] = jnp.zeros_like(send)

    def prepare(j):
        slot = j % 2
        for ch in range(chunks):
            at = ch * CHUNK
            lhs_ref[slot, :, at : at + CHUNK] = jnp.transpose(s_ref[j, at : at + CHUNK, :])
        for part in range(2):
            rhs_ref[slot, part] = e_ref[j, :, part * LANES : (part + 1) * LANES].astype(F32)

    def product(j, a):
        slot = j % 2
        off = SEG_ROWS - a
        g = None
        for ch in range(chunks):
            at = ch * CHUNK + off
            rhs = jnp.concatenate([rhs_ref[slot, part, at : at + CHUNK, :] for part in range(2)], 1)
            term = mm(lhs_ref[slot, :, ch * CHUNK : (ch + 1) * CHUNK], rhs.astype(BF16))
            g = term if g is None else g + term
        return (
            g[:LANES, :LANES] + g[LANES:, LANES:],
            g[LANES:, :LANES] - g[:LANES, LANES:],
        )

    lower = iota((LANES, LANES), 1) <= iota((LANES, LANES), 0)

    def fold(j, a, here, later):
        for part in range(2):
            x = jnp.where(lower, here[part], later[part])
            half = LANES // 2
            while half >= 8:
                x = x[:half] + pltpu.roll(x[half:], LANES - half, 1)
                half //= 2
            at = (part * SEG_ROWS + a) * 8
            diag_ref[j % 2, at : at + 8, :] = x

    def finish(j):
        lines = 2 * SEG_ROWS
        x = jnp.concatenate([diag_ref[j % 2, pl.ds(sub, lines, stride=8), :] for sub in range(8)], 1)
        high, low = split(x)
        shift = walk_ref[j] + REACH
        place = iota((8 * LANES, LANES), 0)
        place = place - place // LANES + iota((8 * LANES, LANES), 1) - shift
        turn = jnp.where((place & (LANES - 1)) == 0, 1.0, 0.0).astype(BF16)
        x = mm(jnp.concatenate([high, low], 0), turn)
        x = x[:lines] + x[lines:]
        lane = iota((SEG_ROWS, LANES), 1)
        label = jnp.full((1, LANES), ids_ref[j], jnp.int32).astype(F32)
        zero = jnp.zeros((1, LANES), F32)
        for part in range(2):
            own = x[part * SEG_ROWS : (part + 1) * SEG_ROWS]
            above = jnp.concatenate([zero, own[: SEG_ROWS - 1]], 0)
            tail = jnp.where(lane[:1] < REACH, own[SEG_ROWS - 1 :], 0.0)
            own = jnp.where(lane < shift, above, own)
            for dev in range(devices):
                first = dev * span // LANES
                for r in range(rows_sent):
                    at = first + r
                    row = own[at : at + 1] if at < SEG_ROWS else tail if at == SEG_ROWS else zero
                    to = part * rows_sent + r
                    send[dev, j, to : to + 1, :] = row
        for dev in range(devices):
            send[dev, j, 2 * rows_sent : 2 * rows_sent + 1, :] = label

    def ship(first, count):
        for k, peer in enumerate(peers):
            pltpu.make_async_remote_copy(
                src_ref=send.at[peer, pl.ds(first, count)],
                dst_ref=got.at[me, pl.ds(first, count)],
                send_sem=send_sem.at[k],
                recv_sem=recv_sem.at[k],
                device_id={"tm": peer},
                device_id_type=MESH,
            ).start()

    for copy in loads[0] + small:
        copy.wait()
    prepare(0)
    for j in range(blocks):
        later = product(j, SEG_ROWS)
        for a in reversed(range(SEG_ROWS)):
            here = product(j, a)
            fold(j, a, here, later)
            later = here
            if a == SEG_ROWS - 4 and j > 0:
                finish(j - 1)
            if a == SEG_ROWS // 2 and j == blocks - 1:
                pl.semaphore_wait(barrier, devices - 1)
                ship(0, blocks - 1)
            if a == 4 and j == 0:
                for copy in sum(loads[1:], []):
                    copy.wait()
            if a == 3 and j + 1 < blocks:
                prepare(j + 1)
    finish(blocks - 1)
    ship(blocks - 1, 1)
    got[me] = send[me]
    for k, peer in enumerate(peers):
        pltpu.make_async_copy(send.at[peer], send.at[peer], send_sem.at[k]).wait()
        giver = lax.rem(me + (devices - 1 - k), devices)
        pltpu.make_async_copy(got.at[giver], got.at[giver], recv_sem.at[k]).wait()
    out_ref[...] = got[...].reshape(out_ref.shape)


def cosine(count):
    wrapped = ((count + DOP // 2) & (DOP - 1)) - DOP // 2
    z = (DOP // 4 - jnp.abs(wrapped)).astype(F32) * (2.0 * math.pi / DOP)
    z2 = z * z
    poly = -1.0 / 39916800.0
    for c in (1.0 / 362880.0, -1.0 / 5040.0, 1.0 / 120.0, -1.0 / 6.0, 1.0):
        poly = poly * z2 + c
    return z * poly


def map_kernel(
    span, total, got, guard_ref, size_ref, dft_high, dft_low, tab_high, tab_low, ker_high, ker_low,
    out_ref, power_ref, coef_ref,
):
    me = lax.axis_index("tm")
    rows_sent = window_rows(span)
    pad = got.shape[0] // total
    if span % LANES == 0:
        lead, width = REACH, span + 2 * REACH
    else:
        width = rows_sent * LANES
        lead = pl.multiple_of(lax.rem(me * span, LANES) + REACH, 8)
    guard = guard_ref[...].astype(F32)
    size = size_ref[...].astype(F32)
    guard = jnp.transpose(jnp.broadcast_to(guard, (LANES, span)))
    outer = guard + jnp.transpose(jnp.broadcast_to(size, (LANES, span)))
    dist = iota((span, LANES), 1).astype(F32)
    inside = jnp.where((dist > guard) & (dist <= outer), 1.0, 0.0).astype(BF16)
    kernel = mm(inside, ker_high[...]) + mm(inside, ker_low[...])
    guard, outer = guard[:, :1], outer[:, :1]
    dist = jnp.abs(iota((span, width), 1) - lead - iota((span, width), 0)).astype(F32)
    band = jnp.where((dist > guard) & (dist <= outer), 1.0, 0.0).astype(BF16)
    spot = (me * span + iota((span, 1), 0)).astype(F32)
    last = (D - 1) - spot
    count = jnp.minimum(spot, outer) - jnp.minimum(spot, guard)
    count = count + jnp.minimum(last, outer) - jnp.minimum(last, guard)
    weight = 1.0 / (count + 2.0 * (outer - guard))

    def lines(at):
        return got[pl.ds(at, total, stride=pad), :]

    parts = [jnp.concatenate([lines(part * rows_sent + r) for r in range(rows_sent)], 1) for part in range(2)]
    stacked = jnp.concatenate(parts, 0)
    ids = lines(2 * rows_sent)[:, :1].astype(jnp.int32)
    turns = ids * iota((total, DOP), 1)
    cos_high, cos_low = split(cosine(turns))
    sin_high, sin_low = split(cosine(turns - DOP // 4))
    mix_re_high = jnp.concatenate([cos_high, sin_high], 0)
    mix_re_low = jnp.concatenate([cos_low, sin_low], 0)
    mix_im_high = jnp.concatenate([-sin_high, cos_high], 0)
    mix_im_low = jnp.concatenate([-sin_low, cos_low], 0)
    corr = jnp.transpose(stacked)[:width]
    corr_high, corr_low = split(corr)
    norm = 1.0 / (total * SEGS * D)
    re = mm(corr_high, mix_re_high) + (mm(corr_low, mix_re_high) + mm(corr_high, mix_re_low))
    im = mm(corr_high, mix_im_high) + (mm(corr_low, mix_im_high) + mm(corr_high, mix_im_low))
    power = (re * re + im * im) * norm
    floor = jnp.sum(corr * corr, axis=1, keepdims=True) * norm
    coef = mm3(power, dft_high[...], dft_low[...])
    if span % LANES == 0:
        power_c = power[lead : lead + span]
        coef_c = coef[lead : lead + span]
        floor_c = floor[lead : lead + span]
    else:
        power_ref[:, :DOP] = power
        power_ref[:, DOP:] = jnp.broadcast_to(floor, (width, LANES))
        coef_ref[...] = coef
        power_c = power_ref[pl.ds(lead, span), :DOP]
        floor_c = power_ref[pl.ds(lead, span), DOP:][:, :1]
        coef_c = coef_ref[pl.ds(lead, span), :]
    coef_high, coef_low = split(coef)
    sums = mm(band, coef_high) + mm(band, coef_low) + coef_c * kernel
    noise = mm3(sums, tab_high[...], tab_low[...]) * weight
    out_ref[...] = (power_c - floor_c) / (0.25 + noise)


def np_split(x):
    high = x.astype(BF16)
    return jnp.asarray(high), jnp.asarray((x - high.astype(np.float64)).astype(BF16))


def tables(total):
    lag, freq = np.arange(total), np.arange(DOP)
    angle = 2.0 * np.pi / DOP * ((lag[:, None] * freq[None, :]) % DOP)
    tab = np.concatenate([np.cos(angle), np.sin(angle)], 0)
    scale = np.where(lag == 0, 1.0, 2.0) / DOP
    dft = tab.T * np.concatenate([scale, scale])[None, :]
    dist = np.arange(LANES)
    ker = 2.0 * np.cos(2.0 * np.pi / DOP * ((dist[:, None] * lag[None, :]) % DOP))
    ker = np.concatenate([ker, ker], 1)
    return (*np_split(dft), *np_split(tab), *np_split(ker))


def body(surveillance, ref_samples, block_ids, walk, cfar_guard, cfar_window):
    blocks, rows_all = surveillance.shape[:2]
    devices = lax.axis_size("tm")
    total = blocks * devices
    span = D // devices
    rows_sent = window_rows(span)
    pad = -(-(2 * rows_sent + 1) // 8) * 8
    send_shape = (devices, blocks, pad, LANES)
    vmem = pl.BlockSpec(memory_space=pltpu.VMEM)
    hbm = pl.BlockSpec(memory_space=pltpu.HBM)
    windows = pl.pallas_call(
        functools.partial(correlate_kernel, span),
        out_shape=jax.ShapeDtypeStruct((total * pad, LANES), F32),
        in_specs=[hbm] * 4,
        out_specs=vmem,
        scratch_shapes=[
            pltpu.SMEM((blocks,), jnp.int32),
            pltpu.SMEM((blocks,), jnp.int32),
            pltpu.VMEM(surveillance.shape, BF16),
            pltpu.VMEM(ref_samples.shape, BF16),
            pltpu.VMEM((2, 2 * LANES, rows_all), BF16),
            pltpu.VMEM((2, 2, ref_samples.shape[1], LANES), F32),
            pltpu.VMEM((2, 2 * SEG_ROWS * 8, LANES), F32),
            pltpu.VMEM(send_shape, F32),
            pltpu.VMEM(send_shape, F32),
            pltpu.SemaphoreType.DMA((2,)),
            pltpu.SemaphoreType.DMA((blocks, 2)),
            pltpu.SemaphoreType.DMA((devices,)),
            pltpu.SemaphoreType.DMA((devices,)),
        ],
        compiler_params=pltpu.CompilerParams(
            collective_id=0, has_side_effects=True, vmem_limit_bytes=VMEM_LIMIT
        ),
        name="correlate",
    )(walk, block_ids, surveillance, ref_samples)
    width = span + 2 * REACH if span % LANES == 0 else rows_sent * LANES
    return pl.pallas_call(
        functools.partial(map_kernel, span, total),
        out_shape=jax.ShapeDtypeStruct((span, DOP), F32),
        in_specs=[vmem] * 9,
        out_specs=vmem,
        scratch_shapes=[
            pltpu.VMEM((width, DOP + LANES), F32),
            pltpu.VMEM((width, 2 * total), F32),
        ],
        compiler_params=pltpu.CompilerParams(vmem_limit_bytes=MAP_LIMIT),
        name="map",
    )(windows, cfar_guard.reshape(1, span), cfar_window.reshape(1, span), *tables(total))


def solution(mesh):
    in_specs = (
        P(("chan", "tm"), None, None),
        P("tm", None, None),
        P("tm"),
        P("tm"),
        P("tm"),
        P("tm"),
    )
    out_specs = P(("chan", "tm"), None)
    return jax.shard_map(body, mesh=mesh, in_specs=in_specs, out_specs=out_specs, check_vma=False)
```

```python
import functools
import math

import numpy as np
import jax
import jax.numpy as jnp
from jax import lax
from jax.experimental import pallas as pl
from jax.experimental.pallas import tpu as pltpu
from jax.sharding import PartitionSpec as P

D = 2048
DOP = 512
SEGS = 64
GUARD_MAX = 8
WIN_MAX = 16
REACH = GUARD_MAX + WIN_MAX
LANES = 128
SEG_ROWS = D // LANES
CHUNK = SEG_ROWS * SEG_ROWS
GROUPS = 4
FINISH_AT = 3
SHIP_AT = 5
LAND_AT = 7
LINES = SEG_ROWS + 8
MAP_LIMIT = 24 * 1024 * 1024
VMEM_LIMIT = 53 * 1024 * 1024
MESH = pl.DeviceIdType.MESH
F32 = jnp.float32
BF16 = jnp.bfloat16


def window_rows(span):
    return max(s % LANES + span + 2 * REACH for s in range(0, D, span)) // LANES + 1


def iota(shape, dim):
    return lax.broadcasted_iota(jnp.int32, shape, dim)


def split(x):
    high = x.astype(BF16)
    return high, (x - high.astype(F32)).astype(BF16)


def mm(a, b, dims=((1,), (0,))):
    return lax.dot_general(a, b, (dims, ((), ())), preferred_element_type=F32)


def correlate_kernel(
    span, walk_hbm, ids_hbm, s_hbm, e_hbm, out_ref,
    walk_ref, ids_ref, s_ref, e_ref, lhs_ref, rhs_ref, hold_ref, diag_ref, send, got,
    small_sem, piece_sem, in_sem, send_sem, recv_sem,
):
    blocks, rows_all = s_hbm.shape[:2]
    chunks = rows_all // CHUNK
    devices = got.shape[0]
    rows_sent = window_rows(span)
    group_rows = SEG_ROWS // GROUPS
    per = devices // GROUPS
    me = lax.axis_index("tm")
    barrier = pltpu.get_barrier_semaphore()
    peers = [lax.rem(me + k, devices) for k in range(1, devices)]
    small = [
        pltpu.make_async_copy(walk_hbm, walk_ref, small_sem.at[0]),
        pltpu.make_async_copy(ids_hbm, ids_ref, small_sem.at[1]),
    ]
    loads = [
        [
            pltpu.make_async_copy(s_hbm.at[j], s_ref.at[j], in_sem.at[j, 0]),
            pltpu.make_async_copy(e_hbm.at[j], e_ref.at[j], in_sem.at[j, 1]),
        ]
        for j in range(1, blocks)
    ]
    pieces = []
    for ch in range(chunks):
        rows = pl.ds(ch * CHUNK, CHUNK)
        tail = pl.ds(ch * CHUNK, CHUNK + (SEG_ROWS if ch == chunks - 1 else 0))
        pieces.append(
            [
                pltpu.make_async_copy(s_hbm.at[0, rows], s_ref.at[0, rows], piece_sem.at[ch, 0]),
                pltpu.make_async_copy(e_hbm.at[0, tail], e_ref.at[0, tail], piece_sem.at[ch, 1]),
            ]
        )
    for copy in sum(pieces, []) + small + sum(loads, []):
        copy.start()
    for peer in peers:
        pl.semaphore_signal(barrier, inc=1, device_id={"tm": peer}, device_id_type=MESH)
    send[...] = jnp.zeros_like(send)
    diag_ref[...] = jnp.zeros_like(diag_ref)

    def prepare_chunk(j, ch):
        at = ch * CHUNK
        flip = jnp.transpose(s_ref[j, at : at + CHUNK, :])
        lhs_ref[j, 2 * ch] = flip[:, :LANES]
        lhs_ref[j, 2 * ch + 1] = flip[:, LANES:]
        end = at + CHUNK + (SEG_ROWS if ch == chunks - 1 else 0)
        for part in range(2):
            rhs_ref[j, part, at:end, :] = e_ref[j, at:end, part * LANES : (part + 1) * LANES].astype(F32)

    def prepare(j):
        for ch in range(chunks):
            prepare_chunk(j, ch)

    def product(j, a):
        off = SEG_ROWS - a
        g = None
        for ch in range(chunks):
            at = ch * CHUNK + off
            rhs = jnp.concatenate([rhs_ref[j, part, at : at + CHUNK, :] for part in range(2)], 1)
            lhs = jnp.concatenate([lhs_ref[j, 2 * ch], lhs_ref[j, 2 * ch + 1]], 1)
            term = mm(lhs, rhs.astype(BF16))
            g = term if g is None else g + term
        return g

    def fold(j, step, g):
        totals = [None, None]
        for i in range(0, LANES, 8):
            k = LANES + i
            pair = (
                g[i : i + 8, :LANES] + g[k : k + 8, LANES:],
                g[k : k + 8, :LANES] - g[i : i + 8, LANES:],
            )
            low = iota((8, LANES), 1) <= iota((8, LANES), 0) + i
            for part in range(2):
                if step > 0:
                    prev = hold_ref[j, part, i : i + 8, :]
                    x = jnp.where(low, prev, pair[part])
                    x = pltpu.roll(x, LANES - i, 1) if i else x
                    totals[part] = x if totals[part] is None else totals[part] + x
                if step < SEG_ROWS:
                    hold_ref[j, part, i : i + 8, :] = pair[part]
        if step > 0:
            for part in range(2):
                x = totals[part]
                for half in (4, 2, 1):
                    x = x + pltpu.roll(pltpu.roll(x, 8 - half, 0), LANES - half, 1)
                diag_ref[j, part, step * 8 : step * 8 + 8, :] = x

    def run(j, step):
        fold(j, step, product(j, step))

    def finish(group, count, chosen):
        lines = -(-(count * group_rows + 2) // 8) * 8
        base = group * group_rows
        late_by = (LANES - iota((lines, LANES), 1)) & (LANES - 1)
        place = (iota((lines, LANES), 0) + base) * LANES + late_by
        for j in chosen:
            shift = walk_ref[j] + REACH
            label = jnp.full((1, LANES), ids_ref[j], jnp.int32).astype(F32)
            for part in range(2):
                y = diag_ref[j, part, pl.ds(base * 8, lines, stride=8), :]
                y = pltpu.roll(y, LANES - shift, 1)
                y = jnp.where(late_by < shift, y, pltpu.roll(y, lines - 1, 0))
                y = jnp.where(place < D + REACH, y, 0.0)
                for e in range(per * count):
                    top = e * span // LANES
                    to = part * rows_sent
                    send[group * per + e, j, to : to + rows_sent, :] = y[top : top + rows_sent]
            for e in range(per * count):
                send[group * per + e, j, 2 * rows_sent : 2 * rows_sent + 1, :] = label

    def ship(group, first, count):
        for dev in range(group * per, (group + 1) * per):

            @pl.when(dev != me)
            def _():
                pltpu.make_async_remote_copy(
                    src_ref=send.at[dev, pl.ds(first, count)],
                    dst_ref=got.at[me, pl.ds(first, count)],
                    send_sem=send_sem.at[dev],
                    recv_sem=recv_sem.at[me],
                    device_id={"tm": dev},
                    device_id_type=MESH,
                ).start()

    for ch in range(chunks):
        for copy in pieces[ch]:
            copy.wait()
        prepare_chunk(0, ch)
    for copy in small:
        copy.wait()
    ends = [group_rows * (k + 1) + 2 for k in range(GROUPS)]
    ends[-1] = SEG_ROWS + 1
    late = list(range(max(blocks - 2, 0), blocks))
    early = list(range(late[0]))
    jobs = []
    for j in early:
        for step in range(SEG_ROWS + 1):
            jobs.append((j, step))
    marks = []
    for k in range(GROUPS):
        for j in late:
            for step in range(ends[k - 1] if k else 0, ends[k]):
                jobs.append((j, step))
        marks.append(len(jobs))

    def deliver(k):
        if k == 0:
            pl.semaphore_wait(barrier, devices - 1)
            ship(0, 0, blocks)
            for group in range(1, GROUPS):
                ship(group, 0, len(early))
        elif k < GROUPS - 2:
            ship(k, late[0], len(late))
        elif k == GROUPS - 2:
            ship(k, late[0], len(late))
            ship(k + 1, late[0], len(late) - 1)
        else:
            ship(k, blocks - 1, 1)

    when = {}

    def plan(at, what):
        when.setdefault(at, []).append(what)

    def land():
        for copy in sum(loads, []):
            copy.wait()
        prepare(1)

    plan(LAND_AT, land)
    for j in range(2, blocks):
        plan((SEG_ROWS + 1) * (j - 2) + SEG_ROWS, functools.partial(prepare, j))
    if early:
        plan(marks[0] - 2, functools.partial(finish, 0, GROUPS, early))
    for k in range(GROUPS - 1):
        plan(marks[k] + FINISH_AT, functools.partial(finish, k, 1, late))
        if k < GROUPS - 2:
            plan(marks[k] + SHIP_AT, functools.partial(deliver, k))
    plan(len(jobs) - 3, functools.partial(finish, GROUPS - 1, 1, late[:-1]))
    plan(len(jobs) - 1, functools.partial(deliver, GROUPS - 2))
    for n, (j, step) in enumerate(jobs):
        run(j, step)
        for what in when.get(n + 1, []):
            what()
    finish(GROUPS - 1, 1, late[-1:])
    deliver(GROUPS - 1)
    got[me] = send[me]
    for peer in peers:
        pltpu.make_async_copy(send.at[peer], send.at[peer], send_sem.at[peer]).wait()
        pltpu.make_async_copy(got.at[peer], got.at[peer], recv_sem.at[peer]).wait()
    out_ref[...] = got[...].reshape(out_ref.shape)


def cosine(count):
    wrapped = ((count + DOP // 2) & (DOP - 1)) - DOP // 2
    z = (DOP // 4 - jnp.abs(wrapped)).astype(F32) * (2.0 * math.pi / DOP)
    z2 = z * z
    poly = -1.0 / 39916800.0
    for c in (1.0 / 362880.0, -1.0 / 5040.0, 1.0 / 120.0, -1.0 / 6.0, 1.0):
        poly = poly * z2 + c
    return z * poly


def map_kernel(
    span, total, got, guard_ref, size_ref, dft, tab, ker,
    out_ref, power_ref, coef_ref,
):
    me = lax.axis_index("tm")
    rows_sent = window_rows(span)
    pad = got.shape[0] // total
    if span % LANES == 0:
        lead, width = REACH, span + 2 * REACH
    else:
        width = rows_sent * LANES
        lead = pl.multiple_of(lax.rem(me * span, LANES) + REACH, 8)
    guard = guard_ref[...].astype(F32)
    size = size_ref[...].astype(F32)
    guard = jnp.transpose(jnp.broadcast_to(guard, (LANES, span)))
    outer = guard + jnp.transpose(jnp.broadcast_to(size, (LANES, span)))
    dist = iota((span, LANES), 1).astype(F32)
    inside = jnp.where((dist > guard) & (dist <= outer), 1.0, 0.0).astype(BF16)
    kernel = mm(inside, ker[...])
    kernel = kernel[:, : 2 * total] + kernel[:, 2 * total :]
    guard, outer = guard[:, :1], outer[:, :1]
    dist = jnp.abs(iota((span, width), 1) - lead - iota((span, width), 0)).astype(F32)
    band = jnp.where((dist > guard) & (dist <= outer), 1.0, 0.0).astype(BF16)
    spot = (me * span + iota((span, 1), 0)).astype(F32)
    last = (D - 1) - spot
    count = jnp.minimum(spot, outer) - jnp.minimum(spot, guard)
    count = count + jnp.minimum(last, outer) - jnp.minimum(last, guard)
    weight = 1.0 / (count + 2.0 * (outer - guard))

    def lines(at):
        return got[pl.ds(at, total, stride=pad), :]

    parts = [jnp.concatenate([lines(part * rows_sent + r) for r in range(rows_sent)], 1) for part in range(2)]
    stacked = jnp.concatenate(split(jnp.concatenate(parts, 0)), 0)
    turn = jnp.where(((iota((LANES, LANES), 0) + iota((LANES, LANES), 1)) & (LANES - 1)) == 0, 1.0, 0.0)
    turn = turn.astype(BF16)
    corr = [mm(turn, stacked[:, r * LANES : (r + 1) * LANES], ((1,), (1,))) for r in range(rows_sent)]
    corr = jnp.concatenate(corr, 0)[:width]
    both = corr.astype(BF16)
    both = jnp.concatenate([both, both[:, : 2 * total]], 1)
    ids = lines(2 * rows_sent)[:, :1].astype(jnp.int32)
    turns = ids * iota((total, DOP), 1)
    cos_high, cos_low = split(cosine(turns))
    sin_high, sin_low = split(cosine(turns - DOP // 4))
    mix_re = jnp.concatenate([cos_high, sin_high, cos_high, sin_high, cos_low, sin_low], 0)
    mix_im = jnp.concatenate([-sin_high, cos_high, -sin_high, cos_high, -sin_low, cos_low], 0)
    norm = 1.0 / (total * SEGS * D)
    re = mm(both, mix_re)
    im = mm(both, mix_im)
    power = (re * re + im * im) * norm
    corr = corr[:, : 2 * total] + corr[:, 2 * total :]
    floor = jnp.sum(corr * corr, axis=1, keepdims=True) * norm
    high, low = split(power)
    coef = mm(high, dft[...])
    coef = coef[:, : 2 * total] + coef[:, 2 * total :] + mm(low, dft[:, : 2 * total])
    if span % LANES == 0:
        power_c = power[lead : lead + span]
        coef_c = coef[lead : lead + span]
        floor_c = floor[lead : lead + span]
    else:
        power_ref[:, :DOP] = power
        power_ref[:, DOP:] = jnp.broadcast_to(floor, (width, LANES))
        coef_ref[...] = coef
        power_c = power_ref[pl.ds(lead, span), :DOP]
        floor_c = power_ref[pl.ds(lead, span), DOP:][:, :1]
        coef_c = coef_ref[pl.ds(lead, span), :]
    sums = mm(band, jnp.concatenate(split(coef), 1))
    sums = sums[:, : 2 * total] + sums[:, 2 * total :] + coef_c * kernel
    high, low = split(sums)
    noise = mm(jnp.concatenate([high, low, high], 1), tab[...]) * weight
    out_ref[...] = (power_c - floor_c) / (0.25 + noise)


def np_split(x):
    high = x.astype(BF16)
    return high, (x - high.astype(np.float64)).astype(BF16)


def tables(total):
    lag, freq = np.arange(total), np.arange(DOP)
    angle = 2.0 * np.pi / DOP * ((lag[:, None] * freq[None, :]) % DOP)
    tab = np.concatenate([np.cos(angle), np.sin(angle)], 0)
    scale = np.where(lag == 0, 1.0, 2.0) / DOP
    dft = tab.T * np.concatenate([scale, scale])[None, :]
    dist = np.arange(LANES)
    ker = 2.0 * np.cos(2.0 * np.pi / DOP * ((dist[:, None] * lag[None, :]) % DOP))
    ker = np.concatenate([ker, ker], 1)
    high, low = np_split(tab)
    stacks = np.concatenate(np_split(dft), 1), np.concatenate([high, high, low], 0), np.concatenate(np_split(ker), 1)
    return [jnp.asarray(stack) for stack in stacks]


def body(surveillance, ref_samples, block_ids, walk, cfar_guard, cfar_window):
    blocks, rows_all = surveillance.shape[:2]
    devices = lax.axis_size("tm")
    total = blocks * devices
    span = D // devices
    rows_sent = window_rows(span)
    pad = -(-(2 * rows_sent + 1) // 8) * 8
    send_shape = (devices, blocks, pad, LANES)
    vmem = pl.BlockSpec(memory_space=pltpu.VMEM)
    hbm = pl.BlockSpec(memory_space=pltpu.HBM)
    windows = pl.pallas_call(
        functools.partial(correlate_kernel, span),
        out_shape=jax.ShapeDtypeStruct((total * pad, LANES), F32),
        in_specs=[hbm] * 4,
        out_specs=vmem,
        scratch_shapes=[
            pltpu.SMEM((blocks,), jnp.int32),
            pltpu.SMEM((blocks,), jnp.int32),
            pltpu.VMEM(surveillance.shape, BF16),
            pltpu.VMEM(ref_samples.shape, BF16),
            pltpu.VMEM((blocks, rows_all // LANES, 2 * LANES, LANES), BF16),
            pltpu.VMEM((blocks, 2, ref_samples.shape[1], LANES), F32),
            pltpu.VMEM((blocks, 2, LANES, LANES), F32),
            pltpu.VMEM((blocks, 2, LINES * 8, LANES), F32),
            pltpu.VMEM(send_shape, F32),
            pltpu.VMEM(send_shape, F32),
            pltpu.SemaphoreType.DMA((2,)),
            pltpu.SemaphoreType.DMA((rows_all // CHUNK, 2)),
            pltpu.SemaphoreType.DMA((blocks, 2)),
            pltpu.SemaphoreType.DMA((devices,)),
            pltpu.SemaphoreType.DMA((devices,)),
        ],
        compiler_params=pltpu.CompilerParams(
            collective_id=0, has_side_effects=True, vmem_limit_bytes=VMEM_LIMIT
        ),
        name="correlate",
    )(walk, block_ids, surveillance, ref_samples)
    width = span + 2 * REACH if span % LANES == 0 else rows_sent * LANES
    return pl.pallas_call(
        functools.partial(map_kernel, span, total),
        out_shape=jax.ShapeDtypeStruct((span, DOP), F32),
        in_specs=[vmem] * 6,
        out_specs=vmem,
        scratch_shapes=[
            pltpu.VMEM((width, DOP + LANES), F32),
            pltpu.VMEM((width, 2 * total), F32),
        ],
        compiler_params=pltpu.CompilerParams(vmem_limit_bytes=MAP_LIMIT),
        name="map",
    )(windows, cfar_guard.reshape(1, span), cfar_window.reshape(1, span), *tables(total))


def solution(mesh):
    in_specs = (
        P(("chan", "tm"), None, None),
        P("tm", None, None),
        P("tm"),
        P("tm"),
        P("tm"),
        P("tm"),
    )
    out_specs = P(("chan", "tm"), None)
    return jax.shard_map(body, mesh=mesh, in_specs=in_specs, out_specs=out_specs, check_vma=False)
```

```python
import functools
import math

import numpy as np
import jax
import jax.numpy as jnp
from jax import lax
from jax.experimental import pallas as pl
from jax.experimental.pallas import tpu as pltpu
from jax.sharding import PartitionSpec as P

D = 2048
DOP = 512
SEGS = 64
GUARD_MAX = 8
WIN_MAX = 16
REACH = GUARD_MAX + WIN_MAX
LANES = 128
SEG_ROWS = D // LANES
CHUNK = SEG_ROWS * SEG_ROWS
GROUPS = 4
PIECES = 4
FINISH_AT = 3
SHIP_AT = 5
LAND_AT = 7
LINES = SEG_ROWS + 8
MAP_LIMIT = 24 * 1024 * 1024
VMEM_LIMIT = 53 * 1024 * 1024
MESH = pl.DeviceIdType.MESH
F32 = jnp.float32
BF16 = jnp.bfloat16


def window_rows(span):
    return max(s % LANES + span + 2 * REACH for s in range(0, D, span)) // LANES + 1


def iota(shape, dim):
    return lax.broadcasted_iota(jnp.int32, shape, dim)


def split(x):
    high = x.astype(BF16)
    return high, (x - high.astype(F32)).astype(BF16)


def mm(a, b, dims=((1,), (0,))):
    return lax.dot_general(a, b, (dims, ((), ())), preferred_element_type=F32)


def correlate_kernel(
    span, walk_hbm, ids_hbm, s_hbm, e_hbm, out_ref,
    walk_ref, ids_ref, s_ref, e_ref, lhs_ref, rhs_ref, hold_ref, diag_ref, send, got,
    small_sem, piece_sem, in_sem, send_sem, recv_sem,
):
    blocks, rows_all = s_hbm.shape[:2]
    chunks = rows_all // CHUNK
    devices = got.shape[0]
    rows_sent = window_rows(span)
    group_rows = SEG_ROWS // GROUPS
    per = devices // GROUPS
    me = lax.axis_index("tm")
    barrier = pltpu.get_barrier_semaphore()
    peers = [lax.rem(me + k, devices) for k in range(1, devices)]
    small = [
        pltpu.make_async_copy(walk_hbm, walk_ref, small_sem.at[0]),
        pltpu.make_async_copy(ids_hbm, ids_ref, small_sem.at[1]),
    ]
    loads = [
        [
            pltpu.make_async_copy(s_hbm.at[j], s_ref.at[j], in_sem.at[j, 0]),
            pltpu.make_async_copy(e_hbm.at[j], e_ref.at[j], in_sem.at[j, 1]),
        ]
        for j in range(1, blocks)
    ]
    pieces = []
    for ch in range(chunks):
        rows = pl.ds(ch * CHUNK, CHUNK)
        tail = pl.ds(ch * CHUNK, CHUNK + (SEG_ROWS if ch == chunks - 1 else 0))
        pieces.append(
            [
                pltpu.make_async_copy(s_hbm.at[0, rows], s_ref.at[0, rows], piece_sem.at[ch, 0]),
                pltpu.make_async_copy(e_hbm.at[0, tail], e_ref.at[0, tail], piece_sem.at[ch, 1]),
            ]
        )
    for copy in sum(pieces, []) + small + sum(loads, []):
        copy.start()
    for peer in peers:
        pl.semaphore_signal(barrier, inc=1, device_id={"tm": peer}, device_id_type=MESH)
    send[...] = jnp.zeros_like(send)
    diag_ref[...] = jnp.zeros_like(diag_ref)

    def prepare_chunk(j, ch):
        at = ch * CHUNK
        flip = jnp.transpose(s_ref[j, at : at + CHUNK, :])
        lhs_ref[j, 2 * ch] = flip[:, :LANES]
        lhs_ref[j, 2 * ch + 1] = flip[:, LANES:]
        end = at + CHUNK + (SEG_ROWS if ch == chunks - 1 else 0)
        for part in range(2):
            rhs_ref[j, part, at:end, :] = e_ref[j, at:end, part * LANES : (part + 1) * LANES].astype(F32)

    def prepare(j):
        for ch in range(chunks):
            prepare_chunk(j, ch)

    def product(j, a):
        off = SEG_ROWS - a
        g = None
        for ch in range(chunks):
            at = ch * CHUNK + off
            rhs = jnp.concatenate([rhs_ref[j, part, at : at + CHUNK, :] for part in range(2)], 1)
            lhs = jnp.concatenate([lhs_ref[j, 2 * ch], lhs_ref[j, 2 * ch + 1]], 1)
            term = mm(lhs, rhs.astype(BF16))
            g = term if g is None else g + term
        return g

    def fold(j, step, g):
        totals = [None, None]
        for i in range(0, LANES, 8):
            k = LANES + i
            pair = (
                g[i : i + 8, :LANES] + g[k : k + 8, LANES:],
                g[k : k + 8, :LANES] - g[i : i + 8, LANES:],
            )
            low = iota((8, LANES), 1) <= iota((8, LANES), 0) + i
            for part in range(2):
                if step > 0:
                    prev = hold_ref[j, part, i : i + 8, :]
                    x = jnp.where(low, prev, pair[part])
                    x = pltpu.roll(x, LANES - i, 1) if i else x
                    totals[part] = x if totals[part] is None else totals[part] + x
                if step < SEG_ROWS:
                    hold_ref[j, part, i : i + 8, :] = pair[part]
        if step > 0:
            for part in range(2):
                x = totals[part]
                for half in (4, 2, 1):
                    x = x + pltpu.roll(pltpu.roll(x, 8 - half, 0), LANES - half, 1)
                diag_ref[j, part, step * 8 : step * 8 + 8, :] = x

    def run(j, step):
        fold(j, step, product(j, step))

    def finish(group, count, chosen):
        lines = -(-(count * group_rows + 2) // 8) * 8
        base = group * group_rows
        late_by = (LANES - iota((lines, LANES), 1)) & (LANES - 1)
        place = (iota((lines, LANES), 0) + base) * LANES + late_by
        for j in chosen:
            shift = walk_ref[j] + REACH
            label = jnp.full((1, LANES), ids_ref[j], jnp.int32).astype(F32)
            for part in range(2):
                y = diag_ref[j, part, pl.ds(base * 8, lines, stride=8), :]
                y = pltpu.roll(y, LANES - shift, 1)
                y = jnp.where(late_by < shift, y, pltpu.roll(y, lines - 1, 0))
                y = jnp.where(place < D + REACH, y, 0.0)
                for e in range(per * count):
                    top = e * span // LANES
                    to = part * rows_sent
                    send[group * per + e, j, to : to + rows_sent, :] = y[top : top + rows_sent]
            for e in range(per * count):
                send[group * per + e, j, 2 * rows_sent : 2 * rows_sent + 1, :] = label

    def ship(group, first, count):
        for dev in range(group * per, (group + 1) * per):

            @pl.when(dev != me)
            def _():
                pltpu.make_async_remote_copy(
                    src_ref=send.at[dev, pl.ds(first, count)],
                    dst_ref=got.at[me, pl.ds(first, count)],
                    send_sem=send_sem.at[dev],
                    recv_sem=recv_sem.at[me],
                    device_id={"tm": dev},
                    device_id_type=MESH,
                ).start()

    for ch in range(chunks):
        for copy in pieces[ch]:
            copy.wait()
        prepare_chunk(0, ch)
    for copy in small:
        copy.wait()
    ends = [group_rows * (k + 1) + 2 for k in range(GROUPS)]
    ends[-1] = SEG_ROWS + 1
    late = list(range(max(blocks - 2, 0), blocks))
    early = list(range(late[0]))
    lead = late[0] - 1
    jobs = [(j, step) for j in early for step in range(SEG_ROWS + 1) if j != lead or step < ends[0]]
    jobs += [(j, step) for j in late for step in range(ends[0])]
    marks = [len(jobs)]
    if early:
        jobs += [(lead, step) for step in range(ends[0], SEG_ROWS + 1)]
    for k in range(1, GROUPS):
        jobs += [(j, step) for j in late for step in range(ends[k - 1], ends[k])]
        marks.append(len(jobs))
    first = early[-1:] + late
    old = early[:-1]

    def deliver(k):
        if k == 0:
            pl.semaphore_wait(barrier, devices - 1)
            ship(0, 0, blocks)
            if old:
                for group in range(1, GROUPS):
                    ship(group, 0, len(old))
        elif k == 1:
            ship(1, first[0], len(first))
            if early:
                for group in range(2, GROUPS):
                    ship(group, lead, 1)
        elif k == GROUPS - 2:
            ship(k, late[0], len(late))
            ship(k + 1, late[0], len(late) - 1)
        else:
            ship(k, blocks - 1, 1)

    when = {}

    def plan(at, what):
        when.setdefault(at, []).append(what)

    def land():
        for copy in sum(loads, []):
            copy.wait()
        prepare(1)

    plan(LAND_AT, land)
    for j in range(2, blocks):
        plan(SEG_ROWS + ends[0] * (j - 2), functools.partial(prepare, j))
    if old:
        plan(SEG_ROWS + 4, functools.partial(finish, 0, GROUPS, old))
    plan(marks[0] + FINISH_AT, functools.partial(finish, 0, 1, first))
    plan(marks[0] + SHIP_AT, functools.partial(deliver, 0))
    if early:
        plan(marks[1] - 3, functools.partial(finish, 1, GROUPS - 1, early[-1:]))
    plan(marks[1] + FINISH_AT, functools.partial(finish, 1, 1, late))
    plan(marks[1] + SHIP_AT, functools.partial(deliver, 1))
    plan(marks[2] + FINISH_AT - 1, functools.partial(finish, 2, 1, late))
    plan(len(jobs) - 3, functools.partial(finish, GROUPS - 1, 1, late[:-1]))
    plan(len(jobs) - 1, functools.partial(deliver, GROUPS - 2))
    for n, (j, step) in enumerate(jobs):
        run(j, step)
        for what in when.get(n + 1, []):
            what()
    finish(GROUPS - 1, 1, late[-1:])
    deliver(GROUPS - 1)
    got[me] = send[me]
    for peer in peers:
        pltpu.make_async_copy(send.at[peer], send.at[peer], send_sem.at[peer]).wait()
        pltpu.make_async_copy(got.at[peer], got.at[peer], recv_sem.at[peer]).wait()
    out_ref[...] = got[...].reshape(out_ref.shape)


def cosine(count):
    wrapped = ((count + DOP // 2) & (DOP - 1)) - DOP // 2
    z = (DOP // 4 - jnp.abs(wrapped)).astype(F32) * (2.0 * math.pi / DOP)
    z2 = z * z
    poly = -1.0 / 39916800.0
    for c in (1.0 / 362880.0, -1.0 / 5040.0, 1.0 / 120.0, -1.0 / 6.0, 1.0):
        poly = poly * z2 + c
    return z * poly


def map_kernel(
    span, total, got, guard_ref, size_ref, dft, tab, ker,
    out_hbm, out_ref, power_ref, coef_ref, out_sem,
):
    me = lax.axis_index("tm")
    rows_sent = window_rows(span)
    pad = got.shape[0] // total
    if span % LANES == 0:
        lead, width = REACH, span + 2 * REACH
    else:
        width = rows_sent * LANES
        lead = pl.multiple_of(lax.rem(me * span, LANES) + REACH, 8)
    guard = guard_ref[...].astype(F32)
    size = size_ref[...].astype(F32)
    guard = jnp.transpose(jnp.broadcast_to(guard, (LANES, span)))
    outer = guard + jnp.transpose(jnp.broadcast_to(size, (LANES, span)))
    dist = iota((span, LANES), 1).astype(F32)
    inside = jnp.where((dist > guard) & (dist <= outer), 1.0, 0.0).astype(BF16)
    kernel = mm(inside, ker[...])
    kernel = kernel[:, : 2 * total] + kernel[:, 2 * total :]
    guard, outer = guard[:, :1], outer[:, :1]
    dist = jnp.abs(iota((span, width), 1) - lead - iota((span, width), 0)).astype(F32)
    band = jnp.where((dist > guard) & (dist <= outer), 1.0, 0.0).astype(BF16)
    spot = (me * span + iota((span, 1), 0)).astype(F32)
    last = (D - 1) - spot
    count = jnp.minimum(spot, outer) - jnp.minimum(spot, guard)
    count = count + jnp.minimum(last, outer) - jnp.minimum(last, guard)
    weight = 1.0 / (count + 2.0 * (outer - guard))

    def lines(at):
        return got[pl.ds(at, total, stride=pad), :]

    parts = [jnp.concatenate([lines(part * rows_sent + r) for r in range(rows_sent)], 1) for part in range(2)]
    stacked = jnp.concatenate(split(jnp.concatenate(parts, 0)), 0)
    turn = jnp.where(((iota((LANES, LANES), 0) + iota((LANES, LANES), 1)) & (LANES - 1)) == 0, 1.0, 0.0)
    turn = turn.astype(BF16)
    corr = [mm(turn, stacked[:, r * LANES : (r + 1) * LANES], ((1,), (1,))) for r in range(rows_sent)]
    corr = jnp.concatenate(corr, 0)[:width]
    both = corr.astype(BF16)
    both = jnp.concatenate([both, both[:, : 2 * total]], 1)
    ids = lines(2 * rows_sent)[:, :1].astype(jnp.int32)
    turns = ids * iota((total, DOP), 1)
    cos_high, cos_low = split(cosine(turns))
    sin_high, sin_low = split(cosine(turns - DOP // 4))
    mix_re = jnp.concatenate([cos_high, sin_high, cos_high, sin_high, cos_low, sin_low], 0)
    mix_im = jnp.concatenate([-sin_high, cos_high, -sin_high, cos_high, -sin_low, cos_low], 0)
    norm = 1.0 / (total * SEGS * D)
    re = mm(both, mix_re)
    im = mm(both, mix_im)
    power = (re * re + im * im) * norm
    corr = corr[:, : 2 * total] + corr[:, 2 * total :]
    floor = jnp.sum(corr * corr, axis=1, keepdims=True) * norm
    high, low = split(power)
    coef = mm(high, dft[...])
    coef = coef[:, : 2 * total] + coef[:, 2 * total :] + mm(low, dft[:, : 2 * total])
    if span % LANES == 0:
        power_c = power[lead : lead + span]
        coef_c = coef[lead : lead + span]
        floor_c = floor[lead : lead + span]
    else:
        power_ref[:, :DOP] = power
        power_ref[:, DOP:] = jnp.broadcast_to(floor, (width, LANES))
        coef_ref[...] = coef
        power_c = power_ref[pl.ds(lead, span), :DOP]
        floor_c = power_ref[pl.ds(lead, span), DOP:][:, :1]
        coef_c = coef_ref[pl.ds(lead, span), :]
    sums = mm(band, jnp.concatenate(split(coef), 1))
    sums = sums[:, : 2 * total] + sums[:, 2 * total :] + coef_c * kernel
    high, low = split(sums)
    noise = mm(jnp.concatenate([high, low, high], 1), tab[...]) * weight
    copies = []
    rows = span // PIECES
    for p in range(PIECES):
        piece = slice(p * rows, (p + 1) * rows)
        out_ref[piece] = (power_c[piece] - floor_c[piece]) / (0.25 + noise[piece])
        at = pl.ds(p * rows, rows)
        copies.append(pltpu.make_async_copy(out_ref.at[at], out_hbm.at[at], out_sem.at[p]))
        copies[-1].start()
    for copy in copies:
        copy.wait()


def np_split(x):
    high = x.astype(BF16)
    return high, (x - high.astype(np.float64)).astype(BF16)


def tables(total):
    lag, freq = np.arange(total), np.arange(DOP)
    angle = 2.0 * np.pi / DOP * ((lag[:, None] * freq[None, :]) % DOP)
    tab = np.concatenate([np.cos(angle), np.sin(angle)], 0)
    scale = np.where(lag == 0, 1.0, 2.0) / DOP
    dft = tab.T * np.concatenate([scale, scale])[None, :]
    dist = np.arange(LANES)
    ker = 2.0 * np.cos(2.0 * np.pi / DOP * ((dist[:, None] * lag[None, :]) % DOP))
    ker = np.concatenate([ker, ker], 1)
    high, low = np_split(tab)
    stacks = np.concatenate(np_split(dft), 1), np.concatenate([high, high, low], 0), np.concatenate(np_split(ker), 1)
    return [jnp.asarray(stack) for stack in stacks]


def body(surveillance, ref_samples, block_ids, walk, cfar_guard, cfar_window):
    blocks, rows_all = surveillance.shape[:2]
    devices = lax.axis_size("tm")
    total = blocks * devices
    span = D // devices
    rows_sent = window_rows(span)
    pad = -(-(2 * rows_sent + 1) // 8) * 8
    send_shape = (devices, blocks, pad, LANES)
    vmem = pl.BlockSpec(memory_space=pltpu.VMEM)
    hbm = pl.BlockSpec(memory_space=pltpu.HBM)
    windows = pl.pallas_call(
        functools.partial(correlate_kernel, span),
        out_shape=jax.ShapeDtypeStruct((total * pad, LANES), F32),
        in_specs=[hbm] * 4,
        out_specs=vmem,
        scratch_shapes=[
            pltpu.SMEM((blocks,), jnp.int32),
            pltpu.SMEM((blocks,), jnp.int32),
            pltpu.VMEM(surveillance.shape, BF16),
            pltpu.VMEM(ref_samples.shape, BF16),
            pltpu.VMEM((blocks, rows_all // LANES, 2 * LANES, LANES), BF16),
            pltpu.VMEM((blocks, 2, ref_samples.shape[1], LANES), F32),
            pltpu.VMEM((blocks, 2, LANES, LANES), F32),
            pltpu.VMEM((blocks, 2, LINES * 8, LANES), F32),
            pltpu.VMEM(send_shape, F32),
            pltpu.VMEM(send_shape, F32),
            pltpu.SemaphoreType.DMA((2,)),
            pltpu.SemaphoreType.DMA((rows_all // CHUNK, 2)),
            pltpu.SemaphoreType.DMA((blocks, 2)),
            pltpu.SemaphoreType.DMA((devices,)),
            pltpu.SemaphoreType.DMA((devices,)),
        ],
        compiler_params=pltpu.CompilerParams(
            collective_id=0, has_side_effects=True, vmem_limit_bytes=VMEM_LIMIT
        ),
        name="correlate",
    )(walk, block_ids, surveillance, ref_samples)
    width = span + 2 * REACH if span % LANES == 0 else rows_sent * LANES
    return pl.pallas_call(
        functools.partial(map_kernel, span, total),
        out_shape=jax.ShapeDtypeStruct((span, DOP), F32),
        in_specs=[vmem] * 6,
        out_specs=hbm,
        scratch_shapes=[
            pltpu.VMEM((span, DOP), F32),
            pltpu.VMEM((width, DOP + LANES), F32),
            pltpu.VMEM((width, 2 * total), F32),
            pltpu.SemaphoreType.DMA((PIECES,)),
        ],
        compiler_params=pltpu.CompilerParams(vmem_limit_bytes=MAP_LIMIT),
        name="map",
    )(windows, cfar_guard.reshape(1, span), cfar_window.reshape(1, span), *tables(total))


def solution(mesh):
    in_specs = (
        P(("chan", "tm"), None, None),
        P("tm", None, None),
        P("tm"),
        P("tm"),
        P("tm"),
        P("tm"),
    )
    out_specs = P(("chan", "tm"), None)
    return jax.shard_map(body, mesh=mesh, in_specs=in_specs, out_specs=out_specs, check_vma=False)
```

```python
import functools
import math

import numpy as np
import jax
import jax.numpy as jnp
from jax import lax
from jax.experimental import pallas as pl
from jax.experimental.pallas import tpu as pltpu
from jax.sharding import PartitionSpec as P

D = 2048
DOP = 512
SEGS = 64
WALK = 64
GUARD_MAX = 8
WIN_MAX = 16
REACH = GUARD_MAX + WIN_MAX
LANES = 128
SEG_ROWS = D // LANES
CHUNK = SEG_ROWS * SEG_ROWS
GROUPS = 4
PIECES = 4
FINISH_AT = 3
SHIP_AT = 5
LAND_AT = 7
LINES = SEG_ROWS + 8
MAP_LIMIT = 24 * 1024 * 1024
VMEM_LIMIT = 53 * 1024 * 1024
MESH = pl.DeviceIdType.MESH
F32 = jnp.float32
BF16 = jnp.bfloat16


def window_rows(span):
    return max(s % LANES + span + 2 * REACH for s in range(0, D, span)) // LANES + 1


def iota(shape, dim):
    return lax.broadcasted_iota(jnp.int32, shape, dim)


def split(x):
    high = x.astype(BF16)
    return high, (x - high.astype(F32)).astype(BF16)


def mm(a, b, dims=((1,), (0,))):
    return lax.dot_general(a, b, (dims, ((), ())), preferred_element_type=F32)


def correlate_kernel(
    span, code_hbm, s_hbm, e_hbm, out_ref,
    code_ref, s_ref, e_ref, lhs_ref, rhs_ref, hold_ref, diag_ref, send, got,
    small_sem, piece_sem, in_sem, send_sem, recv_sem,
):
    blocks, rows_all = s_hbm.shape[:2]
    chunks = rows_all // CHUNK
    devices = got.shape[0]
    rows_sent = window_rows(span)
    group_rows = SEG_ROWS // GROUPS
    per = devices // GROUPS
    me = lax.axis_index("tm")
    barrier = pltpu.get_barrier_semaphore()
    peers = [lax.rem(me + k, devices) for k in range(1, devices)]
    small = [pltpu.make_async_copy(code_hbm, code_ref, small_sem.at[0])]
    loads = [
        [
            pltpu.make_async_copy(s_hbm.at[j], s_ref.at[j], in_sem.at[j, 0]),
            pltpu.make_async_copy(e_hbm.at[j], e_ref.at[j], in_sem.at[j, 1]),
        ]
        for j in range(1, blocks)
    ]
    pieces = []
    for ch in range(chunks):
        rows = pl.ds(ch * CHUNK, CHUNK)
        tail = pl.ds(ch * CHUNK, CHUNK + (SEG_ROWS if ch == chunks - 1 else 0))
        pieces.append(
            [
                pltpu.make_async_copy(s_hbm.at[0, rows], s_ref.at[0, rows], piece_sem.at[ch, 0]),
                pltpu.make_async_copy(e_hbm.at[0, tail], e_ref.at[0, tail], piece_sem.at[ch, 1]),
            ]
        )
    for copy in sum(pieces, []) + small + sum(loads, []):
        copy.start()
    for peer in peers:
        pl.semaphore_signal(barrier, inc=1, device_id={"tm": peer}, device_id_type=MESH)
    send[...] = jnp.zeros_like(send)
    diag_ref[...] = jnp.zeros_like(diag_ref)

    def prepare_chunk(j, ch):
        at = ch * CHUNK
        flip = jnp.transpose(s_ref[j, at : at + CHUNK, :])
        lhs_ref[j, 2 * ch] = flip[:, :LANES]
        lhs_ref[j, 2 * ch + 1] = flip[:, LANES:]
        end = at + CHUNK + (SEG_ROWS if ch == chunks - 1 else 0)
        for part in range(2):
            rhs_ref[j, part, at:end, :] = e_ref[j, at:end, part * LANES : (part + 1) * LANES].astype(F32)

    def prepare(j):
        for ch in range(chunks):
            prepare_chunk(j, ch)

    def product(j, a):
        off = SEG_ROWS - a
        g = None
        for ch in range(chunks):
            at = ch * CHUNK + off
            rhs = jnp.concatenate([rhs_ref[j, part, at : at + CHUNK, :] for part in range(2)], 1)
            lhs = jnp.concatenate([lhs_ref[j, 2 * ch], lhs_ref[j, 2 * ch + 1]], 1)
            term = mm(lhs, rhs.astype(BF16))
            g = term if g is None else g + term
        return g

    def fold(j, step, g):
        totals = [None, None]
        for i in range(0, LANES, 8):
            k = LANES + i
            pair = (
                g[i : i + 8, :LANES] + g[k : k + 8, LANES:],
                g[k : k + 8, :LANES] - g[i : i + 8, LANES:],
            )
            low = iota((8, LANES), 1) <= iota((8, LANES), 0) + i
            for part in range(2):
                if step > 0:
                    prev = hold_ref[j, part, i : i + 8, :]
                    x = jnp.where(low, prev, pair[part])
                    x = pltpu.roll(x, LANES - i, 1) if i else x
                    totals[part] = x if totals[part] is None else totals[part] + x
                if step < SEG_ROWS:
                    hold_ref[j, part, i : i + 8, :] = pair[part]
        if step > 0:
            for part in range(2):
                x = totals[part]
                for half in (4, 2, 1):
                    x = x + pltpu.roll(pltpu.roll(x, 8 - half, 0), LANES - half, 1)
                diag_ref[j, part, step * 8 : step * 8 + 8, :] = x

    def run(j, step):
        fold(j, step, product(j, step))

    def finish(group, count, chosen):
        lines = -(-(count * group_rows + 2) // 8) * 8
        base = group * group_rows
        late_by = (LANES - iota((lines, LANES), 1)) & (LANES - 1)
        place = (iota((lines, LANES), 0) + base) * LANES + late_by
        for j in chosen:
            shift = (code_ref[j] & (WALK - 1)) + REACH
            label = jnp.full((1, LANES), code_ref[j] >> (WALK.bit_length() - 1), jnp.int32).astype(F32)
            for part in range(2):
                y = diag_ref[j, part, pl.ds(base * 8, lines, stride=8), :]
                y = pltpu.roll(y, LANES - shift, 1)
                y = jnp.where(late_by < shift, y, pltpu.roll(y, lines - 1, 0))
                y = jnp.where(place < D + REACH, y, 0.0)
                for e in range(per * count):
                    top = e * span // LANES
                    to = part * rows_sent
                    send[group * per + e, j, to : to + rows_sent, :] = y[top : top + rows_sent]
            for e in range(per * count):
                send[group * per + e, j, 2 * rows_sent : 2 * rows_sent + 1, :] = label

    def ship(group, first, count):
        for dev in range(group * per, (group + 1) * per):

            @pl.when(dev != me)
            def _():
                pltpu.make_async_remote_copy(
                    src_ref=send.at[dev, pl.ds(first, count)],
                    dst_ref=got.at[me, pl.ds(first, count)],
                    send_sem=send_sem.at[dev],
                    recv_sem=recv_sem.at[me],
                    device_id={"tm": dev},
                    device_id_type=MESH,
                ).start()

    for ch in range(chunks):
        for copy in pieces[ch]:
            copy.wait()
        prepare_chunk(0, ch)
    for copy in small:
        copy.wait()
    ends = [group_rows * (k + 1) + 2 for k in range(GROUPS)]
    ends[-1] = SEG_ROWS + 1
    late = list(range(max(blocks - 2, 0), blocks))
    early = list(range(late[0]))
    lead = late[0] - 1
    jobs = [(j, step) for j in early for step in range(SEG_ROWS + 1) if j != lead or step < ends[0]]
    jobs += [(j, step) for j in late for step in range(ends[0])]
    marks = [len(jobs)]
    if early:
        jobs += [(lead, step) for step in range(ends[0], SEG_ROWS + 1)]
    for k in range(1, GROUPS):
        jobs += [(j, step) for j in late for step in range(ends[k - 1], ends[k])]
        marks.append(len(jobs))
    first = early[-1:] + late
    old = early[:-1]

    def deliver(k):
        if k == 0:
            pl.semaphore_wait(barrier, devices - 1)
            ship(0, 0, blocks)
            if old:
                for group in range(1, GROUPS):
                    ship(group, 0, len(old))
        elif k == 1:
            ship(1, first[0], len(first))
            if early:
                for group in range(2, GROUPS):
                    ship(group, lead, 1)
        elif k == GROUPS - 2:
            ship(k, late[0], len(late))
            ship(k + 1, late[0], len(late) - 1)
        else:
            ship(k, blocks - 1, 1)

    when = {}

    def plan(at, what):
        when.setdefault(at, []).append(what)

    def land():
        for copy in sum(loads, []):
            copy.wait()
        prepare(1)

    plan(LAND_AT, land)
    for j in range(2, blocks):
        plan(SEG_ROWS + ends[0] * (j - 2), functools.partial(prepare, j))
    if old:
        plan(SEG_ROWS + 4, functools.partial(finish, 0, GROUPS, old))
    plan(marks[0] + FINISH_AT, functools.partial(finish, 0, 1, first))
    plan(marks[0] + SHIP_AT, functools.partial(deliver, 0))
    if early:
        plan(marks[1] - 3, functools.partial(finish, 1, GROUPS - 1, early[-1:]))
    plan(marks[1] + FINISH_AT, functools.partial(finish, 1, 1, late))
    plan(marks[1] + SHIP_AT, functools.partial(deliver, 1))
    plan(marks[2] + FINISH_AT - 1, functools.partial(finish, 2, 1, late))
    plan(len(jobs) - 3, functools.partial(finish, GROUPS - 1, 1, late[:-1]))
    plan(len(jobs) - 1, functools.partial(deliver, GROUPS - 2))
    for n, (j, step) in enumerate(jobs):
        run(j, step)
        for what in when.get(n + 1, []):
            what()
    finish(GROUPS - 1, 1, late[-1:])
    deliver(GROUPS - 1)
    got[me] = send[me]
    for peer in peers:
        pltpu.make_async_copy(send.at[peer], send.at[peer], send_sem.at[peer]).wait()
        pltpu.make_async_copy(got.at[peer], got.at[peer], recv_sem.at[peer]).wait()
    out_ref[...] = got[...].reshape(out_ref.shape)


def cosine(count):
    wrapped = ((count + DOP // 2) & (DOP - 1)) - DOP // 2
    z = (DOP // 4 - jnp.abs(wrapped)).astype(F32) * (2.0 * math.pi / DOP)
    z2 = z * z
    poly = -1.0 / 39916800.0
    for c in (1.0 / 362880.0, -1.0 / 5040.0, 1.0 / 120.0, -1.0 / 6.0, 1.0):
        poly = poly * z2 + c
    return z * poly


def map_kernel(
    span, total, got, guard_ref, size_ref, dft, tab, ker,
    out_hbm, out_ref, power_ref, coef_ref, out_sem,
):
    me = lax.axis_index("tm")
    rows_sent = window_rows(span)
    pad = got.shape[0] // total
    if span % LANES == 0:
        lead, width = REACH, span + 2 * REACH
    else:
        width = rows_sent * LANES
        lead = pl.multiple_of(lax.rem(me * span, LANES) + REACH, 8)
    guard = guard_ref[...].astype(F32)
    size = size_ref[...].astype(F32)
    guard = jnp.transpose(jnp.broadcast_to(guard, (LANES, span)))
    outer = guard + jnp.transpose(jnp.broadcast_to(size, (LANES, span)))
    dist = iota((span, LANES), 1).astype(F32)
    inside = jnp.where((dist > guard) & (dist <= outer), 1.0, 0.0).astype(BF16)
    kernel = mm(inside, ker[...])
    kernel = kernel[:, : 2 * total] + kernel[:, 2 * total :]
    guard, outer = guard[:, :1], outer[:, :1]
    dist = jnp.abs(iota((span, width), 1) - lead - iota((span, width), 0)).astype(F32)
    band = jnp.where((dist > guard) & (dist <= outer), 1.0, 0.0).astype(BF16)
    spot = (me * span + iota((span, 1), 0)).astype(F32)
    last = (D - 1) - spot
    count = jnp.minimum(spot, outer) - jnp.minimum(spot, guard)
    count = count + jnp.minimum(last, outer) - jnp.minimum(last, guard)
    weight = 1.0 / (count + 2.0 * (outer - guard))

    def lines(at):
        return got[pl.ds(at, total, stride=pad), :]

    parts = [jnp.concatenate([lines(part * rows_sent + r) for r in range(rows_sent)], 1) for part in range(2)]
    stacked = jnp.concatenate(split(jnp.concatenate(parts, 0)), 0)
    turn = jnp.where(((iota((LANES, LANES), 0) + iota((LANES, LANES), 1)) & (LANES - 1)) == 0, 1.0, 0.0)
    turn = turn.astype(BF16)
    corr = [mm(turn, stacked[:, r * LANES : (r + 1) * LANES], ((1,), (1,))) for r in range(rows_sent)]
    corr = jnp.concatenate(corr, 0)[:width]
    both = corr.astype(BF16)
    both = jnp.concatenate([both, both[:, : 2 * total]], 1)
    ids = lines(2 * rows_sent)[:, :1].astype(jnp.int32)
    turns = ids * iota((total, DOP), 1)
    cos_high, cos_low = split(cosine(turns))
    sin_high, sin_low = split(cosine(turns - DOP // 4))
    mix_re = jnp.concatenate([cos_high, sin_high, cos_high, sin_high, cos_low, sin_low], 0)
    mix_im = jnp.concatenate([-sin_high, cos_high, -sin_high, cos_high, -sin_low, cos_low], 0)
    norm = 1.0 / (total * SEGS * D)
    re = mm(both, mix_re)
    im = mm(both, mix_im)
    power = (re * re + im * im) * norm
    corr = corr[:, : 2 * total] + corr[:, 2 * total :]
    floor = jnp.sum(corr * corr, axis=1, keepdims=True) * norm
    high, low = split(power)
    coef = mm(high, dft[...])
    coef = coef[:, : 2 * total] + coef[:, 2 * total :] + mm(low, dft[:, : 2 * total])
    if span % LANES == 0:
        power_c = power[lead : lead + span]
        coef_c = coef[lead : lead + span]
        floor_c = floor[lead : lead + span]
    else:
        power_ref[:, :DOP] = power
        power_ref[:, DOP:] = jnp.broadcast_to(floor, (width, LANES))
        coef_ref[...] = coef
        power_c = power_ref[pl.ds(lead, span), :DOP]
        floor_c = power_ref[pl.ds(lead, span), DOP:][:, :1]
        coef_c = coef_ref[pl.ds(lead, span), :]
    sums = mm(band, jnp.concatenate(split(coef), 1))
    sums = sums[:, : 2 * total] + sums[:, 2 * total :] + coef_c * kernel
    high, low = split(sums)
    noise = mm(jnp.concatenate([high, low, high], 1), tab[...]) * weight
    copies = []
    rows = span // PIECES
    for p in range(PIECES):
        piece = slice(p * rows, (p + 1) * rows)
        out_ref[piece] = (power_c[piece] - floor_c[piece]) / (0.25 + noise[piece])
        at = pl.ds(p * rows, rows)
        copies.append(pltpu.make_async_copy(out_ref.at[at], out_hbm.at[at], out_sem.at[p]))
        copies[-1].start()
    for copy in copies:
        copy.wait()


def np_split(x):
    high = x.astype(BF16)
    return high, (x - high.astype(np.float64)).astype(BF16)


def tables(total):
    lag, freq = np.arange(total), np.arange(DOP)
    angle = 2.0 * np.pi / DOP * ((lag[:, None] * freq[None, :]) % DOP)
    tab = np.concatenate([np.cos(angle), np.sin(angle)], 0)
    scale = np.where(lag == 0, 1.0, 2.0) / DOP
    dft = tab.T * np.concatenate([scale, scale])[None, :]
    dist = np.arange(LANES)
    ker = 2.0 * np.cos(2.0 * np.pi / DOP * ((dist[:, None] * lag[None, :]) % DOP))
    ker = np.concatenate([ker, ker], 1)
    high, low = np_split(tab)
    stacks = np.concatenate(np_split(dft), 1), np.concatenate([high, high, low], 0), np.concatenate(np_split(ker), 1)
    return [jnp.asarray(stack) for stack in stacks]


def body(surveillance, ref_samples, block_ids, walk, cfar_guard, cfar_window):
    blocks, rows_all = surveillance.shape[:2]
    devices = lax.axis_size("tm")
    total = blocks * devices
    span = D // devices
    rows_sent = window_rows(span)
    pad = -(-(2 * rows_sent + 1) // 8) * 8
    send_shape = (devices, blocks, pad, LANES)
    vmem = pl.BlockSpec(memory_space=pltpu.VMEM)
    hbm = pl.BlockSpec(memory_space=pltpu.HBM)
    windows = pl.pallas_call(
        functools.partial(correlate_kernel, span),
        out_shape=jax.ShapeDtypeStruct((total * pad, LANES), F32),
        in_specs=[hbm] * 3,
        out_specs=vmem,
        scratch_shapes=[
            pltpu.SMEM((blocks,), jnp.int32),
            pltpu.VMEM(surveillance.shape, BF16),
            pltpu.VMEM(ref_samples.shape, BF16),
            pltpu.VMEM((blocks, rows_all // LANES, 2 * LANES, LANES), BF16),
            pltpu.VMEM((blocks, 2, ref_samples.shape[1], LANES), F32),
            pltpu.VMEM((blocks, 2, LANES, LANES), F32),
            pltpu.VMEM((blocks, 2, LINES * 8, LANES), F32),
            pltpu.VMEM(send_shape, F32),
            pltpu.VMEM(send_shape, F32),
            pltpu.SemaphoreType.DMA((1,)),
            pltpu.SemaphoreType.DMA((rows_all // CHUNK, 2)),
            pltpu.SemaphoreType.DMA((blocks, 2)),
            pltpu.SemaphoreType.DMA((devices,)),
            pltpu.SemaphoreType.DMA((devices,)),
        ],
        compiler_params=pltpu.CompilerParams(
            collective_id=0, has_side_effects=True, vmem_limit_bytes=VMEM_LIMIT
        ),
        name="correlate",
    )(block_ids * WALK + walk, surveillance, ref_samples)
    width = span + 2 * REACH if span % LANES == 0 else rows_sent * LANES
    return pl.pallas_call(
        functools.partial(map_kernel, span, total),
        out_shape=jax.ShapeDtypeStruct((span, DOP), F32),
        in_specs=[vmem] * 6,
        out_specs=hbm,
        scratch_shapes=[
            pltpu.VMEM((span, DOP), F32),
            pltpu.VMEM((width, DOP + LANES), F32),
            pltpu.VMEM((width, 2 * total), F32),
            pltpu.SemaphoreType.DMA((PIECES,)),
        ],
        compiler_params=pltpu.CompilerParams(vmem_limit_bytes=MAP_LIMIT),
        name="map",
    )(windows, cfar_guard.reshape(1, span), cfar_window.reshape(1, span), *tables(total))


def solution(mesh):
    in_specs = (
        P(("chan", "tm"), None, None),
        P("tm", None, None),
        P("tm"),
        P("tm"),
        P("tm"),
        P("tm"),
    )
    out_specs = P(("chan", "tm"), None)
    return jax.shard_map(body, mesh=mesh, in_specs=in_specs, out_specs=out_specs, check_vma=False)
```
